32 devices in a mesh: lat: 4 (over z), lon: 8 (over y, x, core).
Axes of the slice: x: 2, y: 2, z: 4, core: 2. Of those that a mesh axis runs over, the one named last changes fastest.
Arguments:
- tracers: bfloat16 [5, 8, 1024, 512], P(None, None, 'lon', 'lat'), may hold values from -6 to 6
- sector_shift: int32 [4], P('lat'), may hold values from 0 to 6, as said below
- lon_offset: int32 [1024, 512], P('lon', 'lat'), may hold values from 2 to 127
- lon_frac: float32 [1024, 512], P('lon', 'lat'), may hold values from 0 to 1
- lat_frac: float32 [1024, 512], P('lon', 'lat'), may hold values from 0 to 1
Outputs:
- advected: bfloat16 [5, 8, 1024, 512], P(None, None, 'lon', 'lat')
The draws below stay inside these ranges and needn't reach their ends.
Inputs may be any that keep to these rules, and one draw needn't show every extreme that they name: `sector_shift`: one count for each band; some band has exactly 6.
All inputs are finite; a program needn't handle non-finite values.
Results may differ from the reference program's by a relative error of at most 0.008.
Values may be sent and summed in bfloat16 or wider, within the bound.
A program may use at most 64 MiB of HBM per device.

```python
import jax
import jax.numpy as jnp
from jax import lax

F = 5
L = 8
CLON = 128
CLAT = 128
SMAX = 6
NLON = 1024
NLAT = 512
NBANDS = 4


def draw_sector_shift(key, part):
    counts = jax.random.randint(jax.random.fold_in(key, 11), (NBANDS,), 0, SMAX + 1)
    chosen = jax.random.randint(jax.random.fold_in(key, 12), (), 0, NBANDS)
    places = jnp.arange(NBANDS, dtype=jnp.int32)
    return jnp.where(places == chosen, SMAX, counts).astype(jnp.int32)


def touch_ends(array, own_key, low, largest):
    longest = array.shape.index(max(array.shape))
    spots = []
    for shift in (0, 1):
        where = [jax.random.randint(jax.random.fold_in(own_key, axis), (), 0, length) for axis, length in enumerate(array.shape)]
        where[longest] = (where[longest] + shift) % array.shape[longest]
        spots.append(tuple(where))
    return array.at[spots[0]].set(low).at[spots[1]].set(largest)


def block_scale(stream_key, dims, shards, least, top_value):
    loudness = 1.0
    for dim, shards_of in shards:
        steps = jax.random.uniform(jax.random.fold_in(jax.random.fold_in(stream_key, 6), dim), (shards_of,), jnp.float32, least / len(shards), top_value / len(shards))
        loudness = loudness * jnp.repeat(jnp.exp(steps), dims[dim] // shards_of).reshape((-1,) + (1,) * (len(dims) - 1 - dim))
    return loudness


def bell_draw(own_key, shape, spread, bound, cuts=(), held_as=jnp.bfloat16):
    array = spread * jax.random.normal(own_key, shape, jnp.float32)
    if cuts:
        array = array * block_scale(own_key, shape, cuts, -0.22, 0.18)
    return jnp.clip(array, -bound, bound).astype(held_as)


def setup_inputs(seed: int = 0) -> dict:
    key_list = jax.random.split(jax.random.key(seed), 6)
    return {
        "tracers": bell_draw(key_list[0], (F, L, NLON, NLAT), 1.0, 6.0, ((2, 8), (3, 4))),
        "sector_shift": draw_sector_shift(jax.random.fold_in(key_list[5], 71), 0),
        "lon_offset": touch_ends(jax.random.randint(key_list[2], (NLON, NLAT), 2, CLON), jax.random.fold_in(key_list[2], 1), 2, CLON - 1).astype(jnp.int32),
        "lon_frac": jnp.clip(1.0 * jax.random.uniform(key_list[3], (NLON, NLAT), jnp.float32) ** block_scale(key_list[3], (NLON, NLAT), ((0, 8), (1, 4)), -0.2, 0.2), 0.0, 1.0),
        "lat_frac": jnp.clip(1.0 * jax.random.uniform(key_list[4], (NLON, NLAT), jnp.float32) ** block_scale(key_list[4], (NLON, NLAT), ((0, 8), (1, 4)), -0.2, 0.2), 0.0, 1.0),
    }


def lagrange(position):
    return (-position * (position - 1.0) * (position - 2.0) / 6.0,
            (position + 1.0) * (position - 1.0) * (position - 2.0) / 2.0,
            -(position + 1.0) * position * (position - 2.0) / 2.0,
            (position + 1.0) * position * (position - 1.0) / 6.0)


def rounded(values):
    return lax.optimization_barrier(values.astype(jnp.bfloat16)).astype(jnp.float32)


def reference(tracers, sector_shift, lon_offset, lon_frac, lat_frac):
    fields, levels = tracers.shape[0], tracers.shape[1]
    shift_rows = jnp.repeat(sector_shift, CLAT, total_repeat_length=NLAT).astype(jnp.int32)
    columns = lax.broadcasted_iota(jnp.int32, (NLON, NLAT), 0)
    base_index = (columns - shift_rows[None, :] * CLON - lon_offset).astype(jnp.int32)
    lon_weights = [rounded(weight) for weight in lagrange(lon_frac)]
    lat_weights = [rounded(weight) for weight in lagrange(lat_frac)]

    def advect(single):
        between = jnp.zeros((NLON, NLAT), jnp.float32)
        for stencil in range(4):
            source = jnp.mod(base_index + (stencil - 1), NLON).astype(jnp.int32)
            picked = jnp.take_along_axis(single, source, axis=0).astype(jnp.float32)
            between = between + lon_weights[stencil] * picked
        between = lax.optimization_barrier(between.astype(jnp.bfloat16))
        padded = jnp.pad(between, ((0, 0), (1, 2))).astype(jnp.float32)
        result = jnp.zeros((NLON, NLAT), jnp.float32)
        for stencil in range(4):
            result = result + lat_weights[stencil] * padded[:, stencil:stencil + NLAT]
        return result.astype(jnp.bfloat16)

    stacked = tracers.reshape(fields * levels, NLON, NLAT)
    return lax.map(advect, stacked).reshape(tracers.shape)
```

```python
import functools

import jax
import jax.numpy as jnp
from jax import lax
from jax.experimental import pallas as pl
from jax.experimental.pallas import tpu as pltpu
from jax.sharding import PartitionSpec as P

SMAX = 6
LANES = 128
EDGE = 16
STEPS = 65535.0
MIDDLE = 32768


def shifted(value, axis, steps):
    count = lax.axis_size(axis)
    pairs = [(source, (source + steps) % count) for source in range(count)]
    return lax.ppermute(value, axis, pairs)


def padded_2(block, sides, width):
    for axis, dim in sides:
        count = lax.axis_size(axis)
        forward = [(i, i + 1) for i in range(count - 1)]
        backward = [(target, source) for source, target in forward]
        low = lax.ppermute(
            lax.slice_in_dim(block, block.shape[dim] - width, None, axis=dim), axis, forward
        )
        high = lax.ppermute(lax.slice_in_dim(block, 0, width, axis=dim), axis, backward)
        block = jnp.concatenate([low, block, high], axis=dim)
    return block


def lagrange(position):
    return (
        -position * (position - 1.0) * (position - 2.0) / 6.0,
        (position + 1.0) * (position - 1.0) * (position - 2.0) / 2.0,
        -(position + 1.0) * position * (position - 2.0) / 2.0,
        (position + 1.0) * position * (position - 1.0) / 6.0,
    )


def general(tracers, sector_shift, lon_offset, lon_frac, lat_frac):
    fields, levels, columns_here, rows_here = tracers.shape
    stacked = tracers.reshape(fields * levels, columns_here, rows_here)
    shift_count = sector_shift[0]
    nothing = jnp.zeros((), jnp.bfloat16)
    lon_weights = [weight.astype(jnp.bfloat16) for weight in lagrange(lon_frac)]
    window_rows = lax.broadcasted_iota(jnp.int32, (2 * columns_here, columns_here, rows_here), 0)
    column_index = lax.broadcasted_iota(jnp.int32, (columns_here, rows_here), 0)
    lon_matrix = jnp.zeros((2 * columns_here, columns_here, rows_here), jnp.bfloat16)
    for stencil in range(4):
        target = column_index - lon_offset + (stencil - 1 + columns_here)
        lon_matrix = lon_matrix + jnp.where(
            window_rows == target[None], lon_weights[stencil][None], nothing
        )
    lat_weights = [weight.astype(jnp.bfloat16).astype(jnp.float32) for weight in lagrange(lat_frac)]
    nearer = stacked
    for bit_place in range(SMAX.bit_length()):
        arrived = shifted(nearer, "lon", 1 << bit_place)
        nearer = jnp.where((shift_count >> bit_place) % 2 == 1, arrived, nearer)
    farther = shifted(nearer, "lon", 1)
    window = jnp.concatenate((farther, nearer), axis=1)
    between = jnp.einsum(
        "bjr,jor->bor", window, lon_matrix, preferred_element_type=jnp.float32
    ).astype(jnp.bfloat16)
    padded = padded_2(between, (("lat", 2),), 2)
    result = jnp.zeros(between.shape, jnp.float32)
    for stencil in range(4):
        result = result + lat_weights[stencil][None] * padded[
            :, :, 1 + stencil : 1 + stencil + rows_here
        ].astype(jnp.float32)
    return result.astype(jnp.bfloat16).reshape(fields, levels, columns_here, rows_here)


def kernel(n, lats, sizes, columns, rows, *refs):
    count = len(sizes)
    starts = [sum(sizes[:chunk]) for chunk in range(count)]
    share = rows // n
    last = count - 1
    shift_ref, tracer_ref, offset_ref, lon_ref, lat_ref, ready = refs[:6]
    refs = refs[6:]
    sent, refs = refs[:count], refs[count:]
    taken, refs = refs[:count], refs[count:]
    mixed, refs = refs[:count], refs[count:]
    home, refs = refs[:count], refs[count:]
    raw, offset, lon_part, lat_part, coded, code, first, lon_weights, lat_weights, wide = refs[:10]
    bottom, top, above, below = refs[10:14]
    (load_sem, part_sem, code_send, code_recv, take_send, take_recv, home_send, home_recv,
     edge_send, edge_recv, rim_send, rim_recv, open_sem) = refs[14:]

    me = lax.axis_index("lon")
    band = lax.axis_index("lat")
    bar = pltpu.get_barrier_semaphore()
    f32, bf16 = jnp.float32, jnp.bfloat16

    def partner(step):
        if n != 8:
            return lax.rem(me + step, n)
        at = step - 1
        mask = (6 - 2 * at + 7 * ((at + 3) // 6)) * (1 - at // 7)
        flips = [lax.rem(mask // bit, 2) for bit in (1, 2, 4)]
        mine = [lax.rem(me // bit, 2) for bit in (1, 2, 4)]
        flips[2] = lax.rem(flips[2] + flips[1] * mine[0], 2)
        return sum(bit * lax.rem(flip + own, 2) for bit, flip, own in zip((1, 2, 4), flips, mine))

    def shared(owner):
        return pl.ds(pl.multiple_of(owner * share, share), share)

    def landed(owner):
        return pl.ds(pl.multiple_of(EDGE + owner * share, EDGE), share)

    def slot(step):
        if n != 8:
            return step
        other = partner(step)
        return sum(bit * lax.rem(other // bit + me // bit, 2) for bit in (1, 2, 4))

    def part_copy(place):
        return pltpu.make_async_copy(
            (offset_ref, lon_ref, lat_ref)[place], (offset, lon_part, lat_part)[place], part_sem.at[place]
        )

    def load_copy(chunk):
        part = pl.ds(starts[chunk], sizes[chunk])
        return pltpu.make_async_copy(tracer_ref.at[part], raw.at[part], load_sem.at[chunk])

    def code_copy(step):
        return pltpu.make_async_remote_copy(
            src_ref=coded.at[:, shared(partner(step))], dst_ref=code.at[me],
            send_sem=code_send.at[slot(step)], recv_sem=code_recv.at[slot(step)],
            device_id={"lon": partner(step)},
        )

    def take_copy(chunk, step):
        return pltpu.make_async_remote_copy(
            src_ref=sent[chunk].at[:, shared(partner(step))], dst_ref=taken[chunk].at[me],
            send_sem=take_send.at[chunk, slot(step)], recv_sem=take_recv.at[chunk, slot(step)],
            device_id={"lon": partner(step)},
        )

    def home_copy(chunk, step):
        return pltpu.make_async_remote_copy(
            src_ref=mixed[chunk].at[partner(step)], dst_ref=home[chunk].at[:, landed(me)],
            send_sem=home_send.at[chunk, slot(step)], recv_sem=home_recv.at[chunk, slot(step)],
            device_id={"lon": partner(step)},
        )

    def edge_up(chunk):
        return pltpu.make_async_remote_copy(
            src_ref=home[chunk].at[:, pl.ds(rows, EDGE)], dst_ref=home[chunk].at[:, pl.ds(0, EDGE)],
            send_sem=edge_send.at[chunk, 0], recv_sem=edge_recv.at[chunk, 0],
            device_id={"lat": band + 1},
        )

    def edge_down(chunk):
        return pltpu.make_async_remote_copy(
            src_ref=home[chunk].at[:, pl.ds(EDGE, EDGE)],
            dst_ref=home[chunk].at[:, pl.ds(EDGE + rows, EDGE)],
            send_sem=edge_send.at[chunk, 1], recv_sem=edge_recv.at[chunk, 1],
            device_id={"lat": band - 1},
        )

    def bottom_copy(sector):
        return pltpu.make_async_remote_copy(
            src_ref=bottom.at[sector], dst_ref=above,
            send_sem=rim_send.at[sector], recv_sem=rim_recv.at[0],
            device_id={"lat": band - 1, "lon": sector},
        )

    def top_copy(sector):
        return pltpu.make_async_remote_copy(
            src_ref=top.at[sector], dst_ref=below,
            send_sem=rim_send.at[sector], recv_sem=rim_recv.at[1],
            device_id={"lat": band + 1, "lon": sector},
        )

    gives_bottom = jnp.logical_and(me == 0, band > 0)
    gives_top = jnp.logical_and(me == n - 1, band < lats - 1)

    for step in range(1, n):
        pl.semaphore_signal(bar, inc=1, device_id={"lon": partner(step)})

    @pl.when(band > 0)
    def _():
        pl.semaphore_signal(bar, inc=1, device_id={"lat": band - 1})

    @pl.when(band < lats - 1)
    def _():
        pl.semaphore_signal(bar, inc=1, device_id={"lat": band + 1})

    load_copy(0).start()
    part_copy(0).start()
    part_copy(1).start()
    for chunk in range(1, count):
        load_copy(chunk).start()
    part_copy(2).start()

    def turn(chunk):
        load_copy(chunk).wait()
        for place in range(sizes[chunk]):
            sent[chunk][place] = raw[starts[chunk] + place].T
        taken[chunk][me] = sent[chunk][:, shared(me)]

    with jax.named_scope("turn0"):
        turn(0)
    part_copy(0).wait()
    part_copy(1).wait()
    coded[0] = offset[...].T.astype(jnp.int16)
    level = jnp.floor(lon_part[...].T * STEPS + 0.5).astype(jnp.int32) - MIDDLE
    coded[1] = level.astype(jnp.int16)
    code[me] = coded[:, shared(me)]

    sides = jnp.where(band > 0, 1, 0) + jnp.where(band < lats - 1, 1, 0)
    with jax.named_scope("bar"):
        pl.semaphore_wait(bar, n - 1 + sides)
    for step in range(1, n):
        code_copy(step).start()
    for chunk in range(count):
        if chunk:
            turn(chunk)
        for step in range(1, n):
            take_copy(chunk, step).start()

    @pl.when(jnp.logical_and(me == 0, band < lats - 1))
    def _():
        pl.semaphore_signal(open_sem, inc=1, device_id={"lat": band + 1})

    @pl.when(jnp.logical_and(me == n - 1, band > 0))
    def _():
        pl.semaphore_signal(open_sem, inc=1, device_id={"lat": band - 1})

    part_copy(2).wait()
    for tap, weight in enumerate(lagrange(lat_part[...].T)):
        lat_weights[tap] = weight.astype(bf16).astype(f32)
    for chunk in range(count):
        @pl.when(band == 0)
        def _():
            home[chunk][:, 0:EDGE] = jnp.zeros((sizes[chunk], EDGE, columns), bf16)

        @pl.when(band == lats - 1)
        def _():
            home[chunk][:, EDGE + rows:] = jnp.zeros((sizes[chunk], EDGE, columns), bf16)

    for step in range(1, n):
        code_copy(step).wait_recv()

    def prepare(sector, carry):
        lane = lax.broadcasted_iota(jnp.int32, (share, columns), 1)
        first[sector] = lane - code[sector, 0].astype(jnp.int32) + (columns - 1)
        level = code[sector, 1].astype(jnp.int32) + MIDDLE
        position = level.astype(f32) * (1.0 / STEPS)
        for tap, weight in enumerate(lagrange(position)):
            lon_weights[tap, sector] = weight.astype(bf16).astype(f32)
        return carry

    lax.fori_loop(0, n, prepare, 0)
    shift_count = shift_ref[0]

    def along_lon(chunk, sector):
        near_at = lax.rem(sector - shift_count + 8 * n, n)
        far_at = lax.rem(sector - shift_count - 1 + 8 * n, n)
        near = [taken[chunk][near_at, place].astype(f32) for place in range(sizes[chunk])]
        far = [taken[chunk][far_at, place].astype(f32) for place in range(sizes[chunk])]
        totals = [[] for _ in near]
        for row in range(0, share, 8):
            part = slice(row, row + 8)
            base = first[sector, part]
            sums = [None] * len(near)
            for tap in range(4):
                spot = base + tap if tap else base
                lane = spot & (columns - 1)
                nearer = spot >= columns
                weight = lon_weights[tap, sector, part]
                for place in range(len(near)):
                    picked = jnp.where(
                        nearer,
                        jnp.take_along_axis(near[place][part], lane, axis=1, mode="promise_in_bounds"),
                        jnp.take_along_axis(far[place][part], lane, axis=1, mode="promise_in_bounds"),
                    )
                    term = weight * picked
                    sums[place] = term if tap == 0 else sums[place] + term
            for place, total in enumerate(sums):
                totals[place].append(total)
        for place, parts in enumerate(totals):
            mixed[chunk][sector, place] = jnp.concatenate(parts, axis=0).astype(bf16)

    for chunk in range(count):
        with jax.named_scope(f"take{chunk}"):
            for step in range(1, n):
                take_copy(chunk, step).wait_recv()

        def send(turn_of, carry):
            step = turn_of
            along_lon(chunk, partner(step))

            @pl.when(step < n)
            def _():
                home_copy(chunk, step).start()
            return carry

        with jax.named_scope(f"lon{chunk}"):
            lax.fori_loop(1, n + 1, send, 0)
        home[chunk][:, landed(me)] = mixed[chunk][me]

    @pl.when(gives_bottom)
    def _():
        pl.semaphore_wait(open_sem, 1)

        def give(sector, carry):
            rows_of = mixed[last][sector].astype(f32)
            for row in range(2):
                bottom[sector, row] = rows_of[:, row].astype(bf16)
            bottom_copy(sector).start()
            return carry

        lax.fori_loop(0, n, give, 0)

    @pl.when(gives_top)
    def _():
        pl.semaphore_wait(open_sem, 1)

        def give(sector, carry):
            top[sector, 0] = mixed[last][sector].astype(f32)[:, share - 1].astype(bf16)
            top_copy(sector).start()
            return carry

        lax.fori_loop(0, n, give, 0)

    def rims():
        @pl.when(band > 0)
        def _():
            top_copy(0).wait_recv()
            row = below[0].astype(f32)
            for place in range(sizes[last]):
                home[last][place, 0:EDGE] = jnp.broadcast_to(
                    row[place : place + 1], (EDGE, columns)
                ).astype(bf16)

        @pl.when(band < lats - 1)
        def _():
            bottom_copy(0).wait_recv()
            near, far = above[0].astype(f32), above[1].astype(f32)
            nearest = lax.broadcasted_iota(jnp.int32, (EDGE, columns), 0) == 0
            for place in range(sizes[last]):
                home[last][place, EDGE + rows :] = jnp.where(
                    nearest, near[place : place + 1], far[place : place + 1]
                ).astype(bf16)

    def along_lat(chunk):
        if chunk < last:
            @pl.when(band > 0)
            def _():
                edge_up(chunk).wait_recv()

            @pl.when(band < lats - 1)
            def _():
                edge_down(chunk).wait_recv()

        def finish(pair, carry):
            for which in range(2):
                place = 2 * pair + which
                wide[which] = home[chunk][place].astype(f32)
                total = lat_weights[0] * wide[which, pl.ds(EDGE - 1, rows)]
                for tap in range(1, 4):
                    total = total + lat_weights[tap] * wide[which, pl.ds(EDGE - 1 + tap, rows)]
                ready[starts[chunk] + place] = total.T.astype(bf16)
            return carry

        with jax.named_scope(f"lat{chunk}"):
            lax.fori_loop(0, sizes[chunk] // 2, finish, 0)

    for step in range(1, n):
        code_copy(step).wait_send()
    for chunk in range(count):
        with jax.named_scope(f"home{chunk}"):
            for step in range(1, n):
                home_copy(chunk, step).wait_recv()

        if chunk < last:
            @pl.when(band > 0)
            def _():
                edge_down(chunk).start()

            @pl.when(band < lats - 1)
            def _():
                edge_up(chunk).start()

            for step in range(1, n):
                take_copy(chunk, step).wait_send()
            if chunk == last - 1:
                with jax.named_scope("rims"):
                    rims()
            if chunk:
                along_lat(chunk - 1)
                if chunk == last - 1:
                    along_lat(chunk)
    along_lat(last)

    with jax.named_scope("sends"):
        for chunk in range(last):
            @pl.when(band > 0)
            def _():
                edge_down(chunk).wait_send()

            @pl.when(band < lats - 1)
            def _():
                edge_up(chunk).wait_send()

            for step in range(1, n):
                home_copy(chunk, step).wait_send()
        for step in range(1, n):
            take_copy(last, step).wait_send()
            home_copy(last, step).wait_send()

        @pl.when(gives_bottom)
        def _():
            for sector in range(n):
                bottom_copy(sector).wait_send()

        @pl.when(gives_top)
        def _():
            for sector in range(n):
                top_copy(sector).wait_send()


def store(parts, ready_ref, out_ref, sem):
    size = ready_ref.shape[0] // parts
    copies = [
        pltpu.make_async_copy(
            ready_ref.at[pl.ds(part * size, size)], out_ref.at[pl.ds(part * size, size)], sem.at[part]
        )
        for part in range(parts)
    ]
    for copy in copies:
        copy.start()
    for copy in copies:
        copy.wait()


def exchanged(tracers, sector_shift, lon_offset, lon_frac, lat_frac):
    fields, levels, columns, rows = tracers.shape
    n, lats = lax.axis_size("lon"), lax.axis_size("lat")
    slices = fields * levels
    leading = [slices // 5 * 2, slices // 5 * 2]
    sizes = [size for size in leading + [slices - sum(leading)] if size]
    share = rows // n
    f32, bf16 = jnp.float32, jnp.bfloat16
    dma = pltpu.SemaphoreType.DMA
    count = len(sizes)
    far = pl.BlockSpec(memory_space=pltpu.HBM)
    scratch = (
        [pltpu.VMEM((size, rows, columns), bf16) for size in sizes]
        + [pltpu.VMEM((n, size, share, columns), bf16) for size in sizes]
        + [pltpu.VMEM((n, size, share, columns), bf16) for size in sizes]
        + [pltpu.VMEM((size, rows + 2 * EDGE, columns), bf16) for size in sizes]
        + [
            pltpu.VMEM((slices, columns, rows), bf16),
            pltpu.VMEM((columns, rows), jnp.int32),
            pltpu.VMEM((columns, rows), f32),
            pltpu.VMEM((columns, rows), f32),
            pltpu.VMEM((2, rows, columns), jnp.int16),
            pltpu.VMEM((n, 2, share, columns), jnp.int16),
            pltpu.VMEM((n, share, columns), jnp.int32),
            pltpu.VMEM((4, n, share, columns), f32),
            pltpu.VMEM((4, rows, columns), f32),
            pltpu.VMEM((2, rows + 2 * EDGE, columns), f32),
            pltpu.VMEM((n, 2, sizes[-1], columns), bf16),
            pltpu.VMEM((n, 1, sizes[-1], columns), bf16),
            pltpu.VMEM((2, sizes[-1], columns), bf16),
            pltpu.VMEM((1, sizes[-1], columns), bf16),
            dma((count,)), dma((3,)),
            dma((n,)), dma((n,)),
            dma((count, n)), dma((count, n)),
            dma((count, n)), dma((count, n)),
            dma((count, 2)), dma((count, 2)),
            dma((n,)), dma((2,)), pltpu.SemaphoreType.REGULAR,
        ]
    )
    ready = pl.pallas_call(
        functools.partial(kernel, n, lats, sizes, columns, rows),
        out_shape=pltpu.VMEM((slices, columns, rows), bf16),
        in_specs=[pl.BlockSpec(memory_space=pltpu.SMEM), far, far, far, far],
        out_specs=pl.BlockSpec(memory_space=pltpu.VMEM),
        scratch_shapes=scratch,
        compiler_params=pltpu.CompilerParams(
            collective_id=0, has_side_effects=True, vmem_limit_bytes=24_000_000
        ),
    )(
        sector_shift,
        *[
            pltpu.with_memory_space_constraint(value, pltpu.HBM)
            for value in (tracers.reshape(slices, columns, rows), lon_offset, lon_frac, lat_frac)
        ],
    )
    parts = 4 if slices % 4 == 0 else 1
    result = pl.pallas_call(
        functools.partial(store, parts),
        out_shape=jax.ShapeDtypeStruct((slices, columns, rows), bf16),
        in_specs=[pl.BlockSpec(memory_space=pltpu.VMEM)],
        out_specs=far,
        scratch_shapes=[dma((parts,))],
        compiler_params=pltpu.CompilerParams(vmem_limit_bytes=4_000_000),
    )(ready)
    return result.reshape(tracers.shape)


def local(tracers, *rest):
    fields, levels, columns, rows = tracers.shape
    split = EDGE * lax.axis_size("lon")
    if columns == LANES and rows == LANES and rows % split == 0 and (fields * levels) % 2 == 0:
        return exchanged(tracers, *rest)
    return general(tracers, *rest)


def solution(mesh):
    return jax.shard_map(
        local,
        mesh=mesh,
        in_specs=(
            P(None, None, "lon", "lat"),
            P("lat"),
            P("lon", "lat"),
            P("lon", "lat"),
            P("lon", "lat"),
        ),
        out_specs=P(None, None, "lon", "lat"),
        check_vma=False,
    )
```

```python
import functools

import jax
import jax.numpy as jnp
from jax import lax
from jax.experimental import pallas as pl
from jax.experimental.pallas import tpu as pltpu
from jax.sharding import PartitionSpec as P

SMAX = 6
LANES = 128
EDGE = 16
STEPS = 65535.0
MIDDLE = 32768
BLOCK = 32
GROUP = 4
PARTS = (4, 3)


def shifted(value, axis, steps):
    count = lax.axis_size(axis)
    pairs = [(source, (source + steps) % count) for source in range(count)]
    return lax.ppermute(value, axis, pairs)


def padded_2(block, sides, width):
    for axis, dim in sides:
        count = lax.axis_size(axis)
        forward = [(i, i + 1) for i in range(count - 1)]
        backward = [(target, source) for source, target in forward]
        low = lax.ppermute(
            lax.slice_in_dim(block, block.shape[dim] - width, None, axis=dim), axis, forward
        )
        high = lax.ppermute(lax.slice_in_dim(block, 0, width, axis=dim), axis, backward)
        block = jnp.concatenate([low, block, high], axis=dim)
    return block


def lagrange(position):
    return (
        -position * (position - 1.0) * (position - 2.0) / 6.0,
        (position + 1.0) * (position - 1.0) * (position - 2.0) / 2.0,
        -(position + 1.0) * position * (position - 2.0) / 2.0,
        (position + 1.0) * position * (position - 1.0) / 6.0,
    )


def general(tracers, sector_shift, lon_offset, lon_frac, lat_frac):
    fields, levels, columns_here, rows_here = tracers.shape
    stacked = tracers.reshape(fields * levels, columns_here, rows_here)
    shift_count = sector_shift[0]
    nothing = jnp.zeros((), jnp.bfloat16)
    lon_weights = [weight.astype(jnp.bfloat16) for weight in lagrange(lon_frac)]
    window_rows = lax.broadcasted_iota(jnp.int32, (2 * columns_here, columns_here, rows_here), 0)
    column_index = lax.broadcasted_iota(jnp.int32, (columns_here, rows_here), 0)
    lon_matrix = jnp.zeros((2 * columns_here, columns_here, rows_here), jnp.bfloat16)
    for stencil in range(4):
        target = column_index - lon_offset + (stencil - 1 + columns_here)
        lon_matrix = lon_matrix + jnp.where(
            window_rows == target[None], lon_weights[stencil][None], nothing
        )
    lat_weights = [weight.astype(jnp.bfloat16).astype(jnp.float32) for weight in lagrange(lat_frac)]
    nearer = stacked
    for bit_place in range(SMAX.bit_length()):
        arrived = shifted(nearer, "lon", 1 << bit_place)
        nearer = jnp.where((shift_count >> bit_place) % 2 == 1, arrived, nearer)
    farther = shifted(nearer, "lon", 1)
    window = jnp.concatenate((farther, nearer), axis=1)
    between = jnp.einsum(
        "bjr,jor->bor", window, lon_matrix, preferred_element_type=jnp.float32
    ).astype(jnp.bfloat16)
    padded = padded_2(between, (("lat", 2),), 2)
    result = jnp.zeros(between.shape, jnp.float32)
    for stencil in range(4):
        result = result + lat_weights[stencil][None] * padded[
            :, :, 1 + stencil : 1 + stencil + rows_here
        ].astype(jnp.float32)
    return result.astype(jnp.bfloat16).reshape(fields, levels, columns_here, rows_here)


def blended(weights_ref, wide, rows):
    totals = [[] for _ in range(wide.shape[0])]
    for row in range(0, rows, BLOCK):
        weights = [weights_ref[tap, row : row + BLOCK] for tap in range(4)]
        for which, parts in enumerate(totals):
            total = weights[0] * wide[which, pl.ds(EDGE - 1 + row, BLOCK)]
            for tap in range(1, 4):
                total = total + weights[tap] * wide[which, pl.ds(EDGE - 1 + tap + row, BLOCK)]
            parts.append(total)
    return [jnp.concatenate(parts, axis=0).astype(jnp.bfloat16).T for parts in totals]


def kernel(n, lats, sizes, columns, rows, *refs):
    count = len(sizes)
    starts = [sum(sizes[:chunk]) for chunk in range(count)]
    share = rows // n
    last = count - 1
    shift_ref, tracer_ref, offset_ref, lon_ref, lat_ref, ready, home_last, lat_weights = refs[:8]
    refs = refs[8:]
    sent, refs = refs[:count], refs[count:]
    taken, refs = refs[:count], refs[count:]
    mixed, refs = refs[:count], refs[count:]
    home, refs = refs[:last] + (home_last,), refs[last:]
    raw, offset, lon_part, lat_part, coded, code, first, lon_weights, wide = refs[:9]
    refs = refs[9:]
    low, refs = refs[:count], refs[count:]
    high, refs = refs[:count], refs[count:]
    above, refs = refs[:count], refs[count:]
    below, refs = refs[:count], refs[count:]
    (load_sem, part_sem, code_send, code_recv, take_send, take_recv, home_send, home_recv,
     edge_send, edge_recv, rim_send, open_sem) = refs

    me = lax.axis_index("lon")
    band = lax.axis_index("lat")
    bar = pltpu.get_barrier_semaphore()
    f32, bf16 = jnp.float32, jnp.bfloat16

    def partner(step):
        if n != 8:
            return lax.rem(me + step, n)
        at = step - 1
        mask = (6 - 2 * at + 7 * ((at + 3) // 6)) * (1 - at // 7)
        flips = [lax.rem(mask // bit, 2) for bit in (1, 2, 4)]
        mine = [lax.rem(me // bit, 2) for bit in (1, 2, 4)]
        flips[2] = lax.rem(flips[2] + flips[1] * mine[0], 2)
        return sum(bit * lax.rem(flip + own, 2) for bit, flip, own in zip((1, 2, 4), flips, mine))

    def shared(owner):
        return pl.ds(pl.multiple_of(owner * share, share), share)

    def landed(owner):
        return pl.ds(pl.multiple_of(EDGE + owner * share, EDGE), share)

    def part_copy(place):
        return pltpu.make_async_copy(
            (offset_ref, lon_ref, lat_ref)[place], (offset, lon_part, lat_part)[place], part_sem.at[place]
        )

    def load_copy(chunk):
        part = pl.ds(starts[chunk], sizes[chunk])
        return pltpu.make_async_copy(tracer_ref.at[part], raw.at[part], load_sem.at[chunk])

    def code_copy(step):
        return pltpu.make_async_remote_copy(
            src_ref=coded.at[:, shared(partner(step))], dst_ref=code.at[me],
            send_sem=code_send, recv_sem=code_recv,
            device_id={"lon": partner(step)},
        )

    def take_copy(chunk, step):
        return pltpu.make_async_remote_copy(
            src_ref=sent[chunk].at[:, shared(partner(step))], dst_ref=taken[chunk].at[me],
            send_sem=take_send.at[chunk], recv_sem=take_recv.at[chunk],
            device_id={"lon": partner(step)},
        )

    def home_copy(chunk, step):
        return pltpu.make_async_remote_copy(
            src_ref=mixed[chunk].at[partner(step)], dst_ref=home[chunk].at[:, landed(me)],
            send_sem=home_send.at[chunk], recv_sem=home_recv.at[chunk],
            device_id={"lon": partner(step)},
        )

    def every(block, send_sem, recv_sem):
        part = block.at[pl.ds(0, n - 1)]
        return pltpu.make_async_remote_copy(
            src_ref=part, dst_ref=part, send_sem=send_sem, recv_sem=recv_sem,
            device_id={"lon": partner(1)},
        )

    def every_code():
        return every(code, code_send, code_recv)

    def every_take(chunk):
        return every(taken[chunk], take_send.at[chunk], take_recv.at[chunk])

    def every_home(chunk):
        return every(mixed[chunk], home_send.at[chunk], home_recv.at[chunk])

    def bottom_edge(chunk):
        return pltpu.make_async_remote_copy(
            src_ref=low[chunk], dst_ref=above[chunk],
            send_sem=edge_send.at[chunk, 0], recv_sem=edge_recv.at[chunk, 0],
            device_id={"lat": band - 1},
        )

    def top_edge(chunk):
        return pltpu.make_async_remote_copy(
            src_ref=high[chunk], dst_ref=below[chunk],
            send_sem=edge_send.at[chunk, 1], recv_sem=edge_recv.at[chunk, 1],
            device_id={"lat": band + 1},
        )

    def bottom_copy(sector):
        return pltpu.make_async_remote_copy(
            src_ref=low[last].at[sector], dst_ref=above[last],
            send_sem=rim_send, recv_sem=edge_recv.at[last, 0],
            device_id={"lat": band - 1, "lon": sector},
        )

    def top_copy(sector):
        return pltpu.make_async_remote_copy(
            src_ref=high[last].at[sector], dst_ref=below[last],
            send_sem=rim_send, recv_sem=edge_recv.at[last, 1],
            device_id={"lat": band + 1, "lon": sector},
        )

    def every_rim(block, peer):
        return pltpu.make_async_remote_copy(
            src_ref=block, dst_ref=block, send_sem=rim_send, recv_sem=edge_recv.at[last, 0],
            device_id={"lat": peer},
        )

    gives_bottom = jnp.logical_and(me == 0, band > 0)
    gives_top = jnp.logical_and(me == n - 1, band < lats - 1)

    for step in range(1, n):
        pl.semaphore_signal(bar, inc=1, device_id={"lon": partner(step)})

    @pl.when(band > 0)
    def _():
        pl.semaphore_signal(bar, inc=1, device_id={"lat": band - 1})

    @pl.when(band < lats - 1)
    def _():
        pl.semaphore_signal(bar, inc=1, device_id={"lat": band + 1})

    part_copy(0).start()
    part_copy(1).start()
    for chunk in range(count):
        load_copy(chunk).start()
    part_copy(2).start()

    def turn(chunk):
        load_copy(chunk).wait()
        for place in range(sizes[chunk]):
            sent[chunk][place] = raw[starts[chunk] + place].T
        taken[chunk][me] = sent[chunk][:, shared(me)]

    part_copy(0).wait()
    part_copy(1).wait()
    coded[0] = offset[...].T.astype(jnp.int16)
    level = jnp.floor(lon_part[...].T * STEPS + 0.5).astype(jnp.int32) - MIDDLE
    coded[1] = level.astype(jnp.int16)
    code[me] = coded[:, shared(me)]

    sides = jnp.where(band > 0, 1, 0) + jnp.where(band < lats - 1, 1, 0)
    with jax.named_scope("bar"):
        pl.semaphore_wait(bar, n - 1 + sides)
    for step in range(1, n):
        code_copy(step).start()
    for chunk in range(count):
        turn(chunk)
        for step in range(1, n):
            take_copy(chunk, step).start()

    @pl.when(jnp.logical_and(me == 0, band < lats - 1))
    def _():
        pl.semaphore_signal(open_sem, inc=1, device_id={"lat": band + 1})

    @pl.when(jnp.logical_and(me == n - 1, band > 0))
    def _():
        pl.semaphore_signal(open_sem, inc=1, device_id={"lat": band - 1})

    part_copy(2).wait()
    for tap, weight in enumerate(lagrange(lat_part[...].T)):
        lat_weights[tap] = weight.astype(bf16).astype(f32)
    for chunk in range(count):
        @pl.when(band == 0)
        def _():
            home[chunk][:, 0:EDGE] = jnp.zeros((sizes[chunk], EDGE, columns), bf16)

        @pl.when(band == lats - 1)
        def _():
            home[chunk][:, EDGE + rows:] = jnp.zeros((sizes[chunk], EDGE, columns), bf16)

    every_code().wait_recv()

    def prepare(sector, carry):
        lane = lax.broadcasted_iota(jnp.int32, (share, columns), 1)
        first[sector] = lane - code[sector, 0].astype(jnp.int32) + (columns - 1)
        level = code[sector, 1].astype(jnp.int32) + MIDDLE
        position = level.astype(f32) * (1.0 / STEPS)
        for tap, weight in enumerate(lagrange(position)):
            lon_weights[tap, sector] = weight.astype(bf16).astype(f32)
        return carry

    lax.fori_loop(0, n, prepare, 0)
    shift_count = shift_ref[0]

    def along_lon(chunk, sector):
        near_at = lax.rem(sector - shift_count + 8 * n, n)
        far_at = lax.rem(sector - shift_count - 1 + 8 * n, n)
        near = [taken[chunk][near_at, place].astype(f32) for place in range(sizes[chunk])]
        far = [taken[chunk][far_at, place].astype(f32) for place in range(sizes[chunk])]
        totals = [[] for _ in near]
        for row in range(0, share, 8):
            part = slice(row, row + 8)
            base = first[sector, part]
            sums = [None] * len(near)
            for tap in range(4):
                spot = base + tap if tap else base
                lane = spot & (columns - 1)
                nearer = spot >= columns
                weight = lon_weights[tap, sector, part]
                for place in range(len(near)):
                    picked = jnp.where(
                        nearer,
                        jnp.take_along_axis(near[place][part], lane, axis=1, mode="promise_in_bounds"),
                        jnp.take_along_axis(far[place][part], lane, axis=1, mode="promise_in_bounds"),
                    )
                    term = weight * picked
                    sums[place] = term if tap == 0 else sums[place] + term
            for place, total in enumerate(sums):
                totals[place].append(total)
        for place, parts in enumerate(totals):
            mixed[chunk][sector, place] = jnp.concatenate(parts, axis=0).astype(bf16)

    for chunk in range(count):
        with jax.named_scope(f"take{chunk}"):
            every_take(chunk).wait_recv()

        def send(turn_of, carry):
            step = turn_of
            along_lon(chunk, partner(step))

            @pl.when(step < n)
            def _():
                home_copy(chunk, step).start()
            return carry

        with jax.named_scope(f"lon{chunk}"):
            lax.fori_loop(1, n + 1, send, 0)
        home[chunk][:, landed(me)] = mixed[chunk][me]

    @pl.when(gives_bottom)
    def _():
        pl.semaphore_wait(open_sem, 1)

        def give(sector, carry):
            rows_of = mixed[last][sector].astype(f32)
            for row in range(2):
                low[last][sector, row] = rows_of[:, row].astype(bf16)
            bottom_copy(sector).start()
            return carry

        lax.fori_loop(0, n, give, 0)

    @pl.when(gives_top)
    def _():
        pl.semaphore_wait(open_sem, 1)

        def give(sector, carry):
            high[last][sector, 0] = mixed[last][sector].astype(f32)[:, share - 1].astype(bf16)
            top_copy(sector).start()
            return carry

        lax.fori_loop(0, n, give, 0)

    def send_edges(chunk):
        @pl.when(band > 0)
        def _():
            rows_of = home[chunk][:, EDGE : 2 * EDGE].astype(f32)
            for row in range(2):
                low[chunk][row] = rows_of[:, row].astype(bf16)
            bottom_edge(chunk).start()

        @pl.when(band < lats - 1)
        def _():
            rows_of = home[chunk][:, rows : EDGE + rows].astype(f32)
            high[chunk][0] = rows_of[:, EDGE - 1].astype(bf16)
            top_edge(chunk).start()

    def take_edges(chunk):
        @pl.when(band > 0)
        def _():
            (top_edge(chunk) if chunk < last else top_copy(0)).wait_recv()
            row = below[chunk][0].astype(f32)
            for place in range(sizes[chunk]):
                home[chunk][place, 0:EDGE] = jnp.broadcast_to(
                    row[place : place + 1], (EDGE, columns)
                ).astype(bf16)

        @pl.when(band < lats - 1)
        def _():
            (bottom_edge(chunk) if chunk < last else bottom_copy(0)).wait_recv()
            near, far = above[chunk][0].astype(f32), above[chunk][1].astype(f32)
            nearest = lax.broadcasted_iota(jnp.int32, (EDGE, columns), 0) == 0
            for place in range(sizes[chunk]):
                home[chunk][place, EDGE + rows :] = jnp.where(
                    nearest, near[place : place + 1], far[place : place + 1]
                ).astype(bf16)

    def along_lat(chunk):
        def finish(group, carry):
            first_place = group * GROUP
            for which in range(GROUP):
                wide[which] = home[chunk][first_place + which].astype(f32)
            for which, block in enumerate(blended(lat_weights, wide, rows)):
                ready[starts[chunk] + first_place + which] = block
            return carry

        with jax.named_scope(f"lat{chunk}"):
            lax.fori_loop(0, sizes[chunk] // GROUP, finish, 0)

    every_code().wait_send()
    for chunk in range(count):
        with jax.named_scope(f"home{chunk}"):
            every_home(chunk).wait_recv()
        if chunk < last:
            send_edges(chunk)
            every_take(chunk).wait_send()
            if chunk == last - 1:
                take_edges(last)
            with jax.named_scope(f"edges{chunk}"):
                take_edges(chunk)
            along_lat(chunk)

    with jax.named_scope("sends"):
        for chunk in range(last):
            @pl.when(band > 0)
            def _():
                bottom_edge(chunk).wait_send()

            @pl.when(band < lats - 1)
            def _():
                top_edge(chunk).wait_send()

            every_home(chunk).wait_send()
        every_take(last).wait_send()
        every_home(last).wait_send()

        @pl.when(gives_bottom)
        def _():
            every_rim(low[last], band - 1).wait_send()

        @pl.when(gives_top)
        def _():
            every_rim(high[last], band + 1).wait_send()


def finishing(rows, ready_ref, home_ref, weights_ref, out_ref, done, wide, sem):
    head, tail = ready_ref.shape[0], home_ref.shape[0]
    sizes = [head // 2, head - head // 2]
    copies = []

    def put(source, place, size):
        copy = pltpu.make_async_copy(source, out_ref.at[pl.ds(place, size)], sem.at[len(copies)])
        copy.start()
        copies.append(copy)

    for part, size in enumerate(sizes):
        place = sum(sizes[:part])
        put(ready_ref.at[pl.ds(place, size)], place, size)
    for group in range(0, tail, GROUP):
        for which in range(GROUP):
            wide[which] = home_ref[group + which].astype(jnp.float32)
        for which, block in enumerate(blended(weights_ref, wide, rows)):
            done[group + which] = block
        put(done.at[pl.ds(group, GROUP)], head + group, GROUP)
    for copy in copies:
        copy.wait()


def exchanged(tracers, sector_shift, lon_offset, lon_frac, lat_frac):
    fields, levels, columns, rows = tracers.shape
    n, lats = lax.axis_size("lon"), lax.axis_size("lat")
    slices = fields * levels
    leading = [slices * part // 40 * GROUP for part in PARTS]
    sizes = [size for size in leading + [slices - sum(leading)] if size]
    share = rows // n
    f32, bf16 = jnp.float32, jnp.bfloat16
    dma = pltpu.SemaphoreType.DMA
    count = len(sizes)
    far = pl.BlockSpec(memory_space=pltpu.HBM)
    scratch = (
        [pltpu.VMEM((size, rows, columns), bf16) for size in sizes]
        + [pltpu.VMEM((n, size, share, columns), bf16) for size in sizes]
        + [pltpu.VMEM((n, size, share, columns), bf16) for size in sizes]
        + [pltpu.VMEM((size, rows + 2 * EDGE, columns), bf16) for size in sizes[:-1]]
        + [
            pltpu.VMEM((slices, columns, rows), bf16),
            pltpu.VMEM((columns, rows), jnp.int32),
            pltpu.VMEM((columns, rows), f32),
            pltpu.VMEM((columns, rows), f32),
            pltpu.VMEM((2, rows, columns), jnp.int16),
            pltpu.VMEM((n, 2, share, columns), jnp.int16),
            pltpu.VMEM((n, share, columns), jnp.int32),
            pltpu.VMEM((4, n, share, columns), f32),
            pltpu.VMEM((GROUP, rows + 2 * EDGE, columns), f32),
        ]
        + [pltpu.VMEM((2, size, columns), bf16) for size in sizes[:-1]]
        + [pltpu.VMEM((n, 2, sizes[-1], columns), bf16)]
        + [pltpu.VMEM((1, size, columns), bf16) for size in sizes[:-1]]
        + [pltpu.VMEM((n, 1, sizes[-1], columns), bf16)]
        + [pltpu.VMEM((2, size, columns), bf16) for size in sizes]
        + [pltpu.VMEM((1, size, columns), bf16) for size in sizes]
        + [
            dma((count,)), dma((3,)),
            dma(()), dma(()),
            dma((count,)), dma((count,)),
            dma((count,)), dma((count,)),
            dma((count - 1, 2)), dma((count, 2)),
            dma(()), pltpu.SemaphoreType.REGULAR,
        ]
    )
    tail = sizes[-1]
    near = pl.BlockSpec(memory_space=pltpu.VMEM)
    parts = pl.pallas_call(
        functools.partial(kernel, n, lats, sizes, columns, rows),
        out_shape=(
            pltpu.VMEM((slices - tail, columns, rows), bf16),
            pltpu.VMEM((tail, rows + 2 * EDGE, columns), bf16),
            pltpu.VMEM((4, rows, columns), f32),
        ),
        in_specs=[pl.BlockSpec(memory_space=pltpu.SMEM), far, far, far, far],
        out_specs=(near,) * 3,
        scratch_shapes=scratch,
        compiler_params=pltpu.CompilerParams(
            collective_id=0, has_side_effects=True, vmem_limit_bytes=24_000_000
        ),
    )(
        sector_shift,
        *[
            pltpu.with_memory_space_constraint(value, pltpu.HBM)
            for value in (tracers.reshape(slices, columns, rows), lon_offset, lon_frac, lat_frac)
        ],
    )
    result = pl.pallas_call(
        functools.partial(finishing, rows),
        out_shape=jax.ShapeDtypeStruct((slices, columns, rows), bf16),
        in_specs=[near] * 3,
        out_specs=far,
        scratch_shapes=[
            pltpu.VMEM((tail, columns, rows), bf16),
            pltpu.VMEM((GROUP, rows + 2 * EDGE, columns), f32),
            dma((2 + tail // GROUP,)),
        ],
        compiler_params=pltpu.CompilerParams(vmem_limit_bytes=8_000_000),
    )(*parts)
    return result.reshape(tracers.shape)


def local(tracers, *rest):
    fields, levels, columns, rows = tracers.shape
    split = EDGE * lax.axis_size("lon")
    if columns == LANES and rows == LANES and rows % split == 0 and (fields * levels) % (10 * GROUP) == 0:
        return exchanged(tracers, *rest)
    return general(tracers, *rest)


def solution(mesh):
    return jax.shard_map(
        local,
        mesh=mesh,
        in_specs=(
            P(None, None, "lon", "lat"),
            P("lat"),
            P("lon", "lat"),
            P("lon", "lat"),
            P("lon", "lat"),
        ),
        out_specs=P(None, None, "lon", "lat"),
        check_vma=False,
    )
```

```python
import functools

import jax
import jax.numpy as jnp
from jax import lax
from jax.experimental import pallas as pl
from jax.experimental.pallas import tpu as pltpu
from jax.sharding import PartitionSpec as P

SMAX = 6
LANES = 128
EDGE = 16
STEPS = 65535.0
MIDDLE = 32768
BLOCK = 32
GROUP = 4
PARTS = (4, 2)


def shifted(value, axis, steps):
    count = lax.axis_size(axis)
    pairs = [(source, (source + steps) % count) for source in range(count)]
    return lax.ppermute(value, axis, pairs)


def padded_2(block, sides, width):
    for axis, dim in sides:
        count = lax.axis_size(axis)
        forward = [(i, i + 1) for i in range(count - 1)]
        backward = [(target, source) for source, target in forward]
        low = lax.ppermute(
            lax.slice_in_dim(block, block.shape[dim] - width, None, axis=dim), axis, forward
        )
        high = lax.ppermute(lax.slice_in_dim(block, 0, width, axis=dim), axis, backward)
        block = jnp.concatenate([low, block, high], axis=dim)
    return block


def lagrange(position):
    return (
        -position * (position - 1.0) * (position - 2.0) / 6.0,
        (position + 1.0) * (position - 1.0) * (position - 2.0) / 2.0,
        -(position + 1.0) * position * (position - 2.0) / 2.0,
        (position + 1.0) * position * (position - 1.0) / 6.0,
    )


def general(tracers, sector_shift, lon_offset, lon_frac, lat_frac):
    fields, levels, columns_here, rows_here = tracers.shape
    stacked = tracers.reshape(fields * levels, columns_here, rows_here)
    shift_count = sector_shift[0]
    nothing = jnp.zeros((), jnp.bfloat16)
    lon_weights = [weight.astype(jnp.bfloat16) for weight in lagrange(lon_frac)]
    window_rows = lax.broadcasted_iota(jnp.int32, (2 * columns_here, columns_here, rows_here), 0)
    column_index = lax.broadcasted_iota(jnp.int32, (columns_here, rows_here), 0)
    lon_matrix = jnp.zeros((2 * columns_here, columns_here, rows_here), jnp.bfloat16)
    for stencil in range(4):
        target = column_index - lon_offset + (stencil - 1 + columns_here)
        lon_matrix = lon_matrix + jnp.where(
            window_rows == target[None], lon_weights[stencil][None], nothing
        )
    lat_weights = [weight.astype(jnp.bfloat16).astype(jnp.float32) for weight in lagrange(lat_frac)]
    nearer = stacked
    for bit_place in range(SMAX.bit_length()):
        arrived = shifted(nearer, "lon", 1 << bit_place)
        nearer = jnp.where((shift_count >> bit_place) % 2 == 1, arrived, nearer)
    farther = shifted(nearer, "lon", 1)
    window = jnp.concatenate((farther, nearer), axis=1)
    between = jnp.einsum(
        "bjr,jor->bor", window, lon_matrix, preferred_element_type=jnp.float32
    ).astype(jnp.bfloat16)
    padded = padded_2(between, (("lat", 2),), 2)
    result = jnp.zeros(between.shape, jnp.float32)
    for stencil in range(4):
        result = result + lat_weights[stencil][None] * padded[
            :, :, 1 + stencil : 1 + stencil + rows_here
        ].astype(jnp.float32)
    return result.astype(jnp.bfloat16).reshape(fields, levels, columns_here, rows_here)


def blended(weights_ref, wide, rows):
    totals = [[] for _ in range(wide.shape[0])]
    for row in range(0, rows, BLOCK):
        weights = [weights_ref[tap, row : row + BLOCK] for tap in range(4)]
        for which, parts in enumerate(totals):
            total = weights[0] * wide[which, pl.ds(EDGE - 1 + row, BLOCK)]
            for tap in range(1, 4):
                total = total + weights[tap] * wide[which, pl.ds(EDGE - 1 + tap + row, BLOCK)]
            parts.append(total)
    return [jnp.concatenate(parts, axis=0).astype(jnp.bfloat16).T for parts in totals]


def kernel(n, lats, sizes, columns, rows, *refs):
    count = len(sizes)
    starts = [sum(sizes[:chunk]) for chunk in range(count)]
    share = rows // n
    last = count - 1
    shift_ref, tracer_ref, offset_ref, lon_ref, lat_ref, ready, home_last, lat_weights = refs[:8]
    refs = refs[8:]
    sent, refs = refs[:count], refs[count:]
    taken, refs = refs[:count], refs[count:]
    mixed, refs = refs[:count], refs[count:]
    home, refs = refs[:last] + (home_last,), refs[last:]
    raw, offset, lon_part, lat_part, coded, code, first, lon_weights, wide = refs[:9]
    refs = refs[9:]
    low, refs = refs[:count], refs[count:]
    high, refs = refs[:count], refs[count:]
    above, refs = refs[:count], refs[count:]
    below, refs = refs[:count], refs[count:]
    relay, refs = refs[0], refs[1:]
    (load_sem, part_sem, code_send, code_recv, take_send, take_recv, home_send, home_recv,
     edge_send, edge_recv, rim_send, rim_recv, open_sem) = refs

    me = lax.axis_index("lon")
    band = lax.axis_index("lat")
    bar = pltpu.get_barrier_semaphore()
    f32, bf16 = jnp.float32, jnp.bfloat16

    def partner(step):
        if n != 8:
            return lax.rem(me + step, n)
        at = step - 1
        pair = 6 - 2 * (at // 2) + at - 2 * (at // 2)
        mask = pair + at // 6 * (1 - 2 * pair)
        flips = [lax.rem(mask // bit, 2) for bit in (1, 2, 4)]
        mine = [lax.rem(me // bit, 2) for bit in (1, 2, 4)]
        flips[2] = lax.rem(flips[2] + flips[1] * mine[0], 2)
        return sum(bit * lax.rem(flip + own, 2) for bit, flip, own in zip((1, 2, 4), flips, mine))

    def shared(owner):
        return pl.ds(pl.multiple_of((n - 1 - owner) * share, share), share)

    def landed(owner):
        return pl.ds(pl.multiple_of(EDGE + (n - 1 - owner) * share, EDGE), share)

    def part_copy(place):
        return pltpu.make_async_copy(
            (offset_ref, lon_ref, lat_ref)[place], (offset, lon_part, lat_part)[place], part_sem
        )

    def every_part():
        parts = lat_weights.at[pl.ds(0, 3)]
        return pltpu.make_async_copy(parts, parts, part_sem)

    def load_copy():
        return pltpu.make_async_copy(tracer_ref, raw, load_sem)

    def code_copy(step):
        return pltpu.make_async_remote_copy(
            src_ref=coded.at[:, shared(partner(step))], dst_ref=code.at[me],
            send_sem=code_send, recv_sem=code_recv,
            device_id={"lon": partner(step)},
        )

    def take_copy(chunk, step):
        return pltpu.make_async_remote_copy(
            src_ref=sent[chunk].at[:, shared(partner(step))], dst_ref=taken[chunk].at[me],
            send_sem=take_send, recv_sem=take_recv.at[chunk],
            device_id={"lon": partner(step)},
        )

    def home_copy(chunk, step):
        return pltpu.make_async_remote_copy(
            src_ref=mixed[chunk].at[partner(step)], dst_ref=home[chunk].at[:, landed(me)],
            send_sem=home_send, recv_sem=home_recv.at[chunk],
            device_id={"lon": partner(step)},
        )

    def every(block, send_sem, recv_sem):
        part = block.at[pl.ds(0, n - 1)]
        return pltpu.make_async_remote_copy(
            src_ref=part, dst_ref=part, send_sem=send_sem, recv_sem=recv_sem,
            device_id={"lon": partner(1)},
        )

    def every_code():
        return every(code, code_send, code_recv)

    def every_take(chunk):
        return every(taken[chunk], take_send, take_recv.at[chunk])

    def every_home(chunk):
        return every(mixed[chunk], home_send, home_recv.at[chunk])

    def every_send(send_sem):
        part = raw.at[pl.ds(0, raw.shape[0] // n * (n - 1))]
        return pltpu.make_async_remote_copy(
            src_ref=part, dst_ref=part, send_sem=send_sem, recv_sem=take_recv.at[0],
            device_id={"lon": partner(1)},
        )

    def bottom_edge(chunk):
        return pltpu.make_async_remote_copy(
            src_ref=low[chunk] if chunk < last else relay, dst_ref=above[chunk],
            send_sem=edge_send.at[chunk, 0], recv_sem=edge_recv.at[chunk, 0],
            device_id={"lat": band - 1},
        )

    def top_edge(chunk):
        return pltpu.make_async_remote_copy(
            src_ref=high[chunk], dst_ref=below[chunk],
            send_sem=edge_send.at[chunk, 1], recv_sem=edge_recv.at[chunk, 1],
            device_id={"lat": band + 1},
        )

    def bottom_copy(step):
        return pltpu.make_async_remote_copy(
            src_ref=low[last].at[partner(step)], dst_ref=relay,
            send_sem=rim_send, recv_sem=rim_recv,
            device_id={"lon": partner(step)},
        )

    def top_copy(sector):
        return pltpu.make_async_remote_copy(
            src_ref=high[last].at[sector], dst_ref=below[last],
            send_sem=rim_send, recv_sem=edge_recv.at[last, 1],
            device_id={"lat": band + 1, "lon": sector},
        )

    def every_top():
        return pltpu.make_async_remote_copy(
            src_ref=high[last], dst_ref=high[last], send_sem=rim_send, recv_sem=edge_recv.at[last, 1],
            device_id={"lat": band + 1},
        )

    gives_bottom = jnp.logical_and(me == n - 1, band > 0)
    gives_top = jnp.logical_and(me == 0, band < lats - 1)

    for step in range(1, n):
        pl.semaphore_signal(bar, inc=1, device_id={"lon": partner(step)})

    @pl.when(band > 0)
    def _():
        pl.semaphore_signal(bar, inc=1, device_id={"lat": band - 1})

    @pl.when(band < lats - 1)
    def _():
        pl.semaphore_signal(bar, inc=1, device_id={"lat": band + 1})

    part_copy(0).start()
    part_copy(1).start()
    part_copy(2).start()
    load_copy().start()

    def turn(chunk):
        for place in range(sizes[chunk]):
            sent[chunk][place] = raw[starts[chunk] + place].T
        taken[chunk][me] = sent[chunk][:, shared(me)]

    every_part().wait()
    coded[0] = offset[...].T.astype(jnp.int16)
    level = jnp.floor(lon_part[...].T * STEPS + 0.5).astype(jnp.int32) - MIDDLE
    coded[1] = level.astype(jnp.int16)
    code[me] = coded[:, shared(me)]

    sides = jnp.where(band > 0, 1, 0) + jnp.where(band < lats - 1, 1, 0)
    with jax.named_scope("bar"):
        pl.semaphore_wait(bar, n - 1 + sides)
    for step in range(1, n):
        code_copy(step).start()
    load_copy().wait()
    for chunk in range(count):
        turn(chunk)
        for step in range(1, n):
            take_copy(chunk, step).start()

    @pl.when(jnp.logical_and(me == 0, band > 0))
    def _():
        pl.semaphore_signal(open_sem, inc=1, device_id={"lat": band - 1})

    for tap, weight in enumerate(lagrange(lat_part[...].T)):
        lat_weights[tap] = weight.astype(bf16).astype(f32)
    for chunk in range(count):
        @pl.when(band == 0)
        def _():
            home[chunk][:, 0:EDGE] = jnp.zeros((sizes[chunk], EDGE, columns), bf16)

        @pl.when(band == lats - 1)
        def _():
            home[chunk][:, EDGE + rows:] = jnp.zeros((sizes[chunk], EDGE, columns), bf16)

    every_code().wait_recv()

    def prepare(sector, carry):
        lane = lax.broadcasted_iota(jnp.int32, (share, columns), 1)
        first[sector] = lane - code[sector, 0].astype(jnp.int32) + (columns - 1)
        level = code[sector, 1].astype(jnp.int32) + MIDDLE
        position = level.astype(f32) * (1.0 / STEPS)
        for tap, weight in enumerate(lagrange(position)):
            lon_weights[tap, sector] = weight.astype(bf16).astype(f32)
        return carry

    lax.fori_loop(0, n, prepare, 0)
    shift_count = shift_ref[0]

    def along_lon(chunk, sector):
        near_at = lax.rem(sector - shift_count + 8 * n, n)
        far_at = lax.rem(sector - shift_count - 1 + 8 * n, n)
        near = [taken[chunk][near_at, place].astype(f32) for place in range(sizes[chunk])]
        far = [taken[chunk][far_at, place].astype(f32) for place in range(sizes[chunk])]
        totals = [[] for _ in near]
        for row in range(0, share, 8):
            part = slice(row, row + 8)
            base = first[sector, part]
            sums = [None] * len(near)
            for tap in range(4):
                spot = base + tap if tap else base
                lane = spot & (columns - 1)
                nearer = spot >= columns
                weight = lon_weights[tap, sector, part]
                for place in range(len(near)):
                    picked = jnp.where(
                        nearer,
                        jnp.take_along_axis(near[place][part], lane, axis=1, mode="promise_in_bounds"),
                        jnp.take_along_axis(far[place][part], lane, axis=1, mode="promise_in_bounds"),
                    )
                    term = weight * picked
                    sums[place] = term if tap == 0 else sums[place] + term
            for place, total in enumerate(sums):
                totals[place].append(total)
        for place, parts in enumerate(totals):
            mixed[chunk][sector, place] = jnp.concatenate(parts, axis=0).astype(bf16)

    for chunk in range(count):
        with jax.named_scope(f"take{chunk}"):
            every_take(chunk).wait_recv()

        def send(turn_of, carry):
            step = turn_of
            along_lon(chunk, partner(step))

            @pl.when(step < n if chunk == 0 else jnp.logical_and(step < n, jnp.logical_not(gives_bottom)))
            def _():
                home_copy(chunk, step).start()
            return carry

        with jax.named_scope(f"lon{chunk}"):
            lax.fori_loop(1, n + 1, send, 0)
        home[chunk][:, landed(me)] = mixed[chunk][me]

    @pl.when(gives_bottom)
    def _():
        def give(step, carry):
            sector = partner(step)
            rows_of = mixed[last][sector].astype(f32)
            for row in range(2):
                low[last][sector, row] = rows_of[:, row].astype(bf16)

            @pl.when(step < n)
            def _():
                bottom_copy(step).start()
            return carry

        lax.fori_loop(1, n + 1, give, 0)
        relay[...] = low[last][me]
        for chunk in range(1, count):
            def late(step, carry):
                home_copy(chunk, step).start()
                return carry

            lax.fori_loop(1, n, late, 0)

    @pl.when(gives_top)
    def _():
        pl.semaphore_wait(open_sem, 1)

        def give(sector, carry):
            high[last][sector, 0] = mixed[last][sector].astype(f32)[:, share - 1].astype(bf16)
            top_copy(sector).start()
            return carry

        lax.fori_loop(0, n, give, 0)

    def send_edges(chunk):
        @pl.when(band > 0)
        def _():
            rows_of = home[chunk][:, EDGE : 2 * EDGE].astype(f32)
            for row in range(2):
                low[chunk][row] = rows_of[:, row].astype(bf16)
            bottom_edge(chunk).start()

        @pl.when(band < lats - 1)
        def _():
            rows_of = home[chunk][:, rows : EDGE + rows].astype(f32)
            high[chunk][0] = rows_of[:, EDGE - 1].astype(bf16)
            top_edge(chunk).start()

    def take_edges(chunk):
        @pl.when(band > 0)
        def _():
            (top_edge(chunk) if chunk < last else top_copy(0)).wait_recv()
            row = below[chunk][0].astype(f32)
            for place in range(sizes[chunk]):
                home[chunk][place, 0:EDGE] = jnp.broadcast_to(
                    row[place : place + 1], (EDGE, columns)
                ).astype(bf16)

        @pl.when(band < lats - 1)
        def _():
            bottom_edge(chunk).wait_recv()
            near, far = above[chunk][0].astype(f32), above[chunk][1].astype(f32)
            nearest = lax.broadcasted_iota(jnp.int32, (EDGE, columns), 0) == 0
            for place in range(sizes[chunk]):
                home[chunk][place, EDGE + rows :] = jnp.where(
                    nearest, near[place : place + 1], far[place : place + 1]
                ).astype(bf16)

    def along_lat(chunk):
        def finish(group, carry):
            first_place = group * GROUP
            for which in range(GROUP):
                wide[which] = home[chunk][first_place + which].astype(f32)
            for which, block in enumerate(blended(lat_weights, wide, rows)):
                ready[starts[chunk] + first_place + which] = block
            return carry

        with jax.named_scope(f"lat{chunk}"):
            lax.fori_loop(0, sizes[chunk] // GROUP, finish, 0)

    every_code().wait_send()
    for chunk in range(count):
        with jax.named_scope(f"home{chunk}"):
            every_home(chunk).wait_recv()
        if chunk < last:
            send_edges(chunk)
            if chunk == 0:
                with jax.named_scope("relay"):
                    @pl.when(jnp.logical_and(band > 0, me < n - 1))
                    def _():
                        bottom_copy(1).wait_recv()

                    @pl.when(band > 0)
                    def _():
                        bottom_edge(last).start()
            if chunk == last - 1:
                take_edges(last)
            with jax.named_scope(f"edges{chunk}"):
                take_edges(chunk)
            along_lat(chunk)

    with jax.named_scope("sends"):
        every_send(take_send).wait_send()
        every_send(home_send).wait_send()
        for chunk in range(count):
            @pl.when(band > 0)
            def _():
                bottom_edge(chunk).wait_send()

            if chunk < last:
                @pl.when(band < lats - 1)
                def _():
                    top_edge(chunk).wait_send()

        @pl.when(gives_bottom)
        def _():
            every(low[last], rim_send, rim_recv).wait_send()

        @pl.when(gives_top)
        def _():
            every_top().wait_send()


def finishing(rows, ready_ref, home_ref, weights_ref, out_ref, done, wide, sem):
    head, tail = ready_ref.shape[0], home_ref.shape[0]
    copies = []

    def put(source, place, size):
        copy = pltpu.make_async_copy(source, out_ref.at[pl.ds(place, size)], sem.at[len(copies)])
        copy.start()
        copies.append(copy)

    put(ready_ref, 0, head)
    for group in range(0, tail, GROUP):
        part = wide.at[pl.ds(group, GROUP)]
        for which in range(GROUP):
            part[which] = home_ref[group + which].astype(jnp.float32)
        for which, block in enumerate(blended(weights_ref, part, rows)):
            done[group + which] = block
        put(done.at[pl.ds(group, GROUP)], head + group, GROUP)
    for copy in copies:
        copy.wait()


def exchanged(tracers, sector_shift, lon_offset, lon_frac, lat_frac):
    fields, levels, columns, rows = tracers.shape
    n, lats = lax.axis_size("lon"), lax.axis_size("lat")
    slices = fields * levels
    leading = [slices * part // 40 * GROUP for part in PARTS]
    sizes = [size for size in leading + [slices - sum(leading)] if size]
    share = rows // n
    f32, bf16 = jnp.float32, jnp.bfloat16
    dma = pltpu.SemaphoreType.DMA
    count = len(sizes)
    far = pl.BlockSpec(memory_space=pltpu.HBM)
    scratch = (
        [pltpu.VMEM((size, rows, columns), bf16) for size in sizes]
        + [pltpu.VMEM((n, size, share, columns), bf16) for size in sizes]
        + [pltpu.VMEM((n, size, share, columns), bf16) for size in sizes]
        + [pltpu.VMEM((size, rows + 2 * EDGE, columns), bf16) for size in sizes[:-1]]
        + [
            pltpu.VMEM((slices, columns, rows), bf16),
            pltpu.VMEM((columns, rows), jnp.int32),
            pltpu.VMEM((columns, rows), f32),
            pltpu.VMEM((columns, rows), f32),
            pltpu.VMEM((2, rows, columns), jnp.int16),
            pltpu.VMEM((n, 2, share, columns), jnp.int16),
            pltpu.VMEM((n, share, columns), jnp.int32),
            pltpu.VMEM((4, n, share, columns), f32),
            pltpu.VMEM((GROUP, rows + 2 * EDGE, columns), f32),
        ]
        + [pltpu.VMEM((2, size, columns), bf16) for size in sizes[:-1]]
        + [pltpu.VMEM((n, 2, sizes[-1], columns), bf16)]
        + [pltpu.VMEM((1, size, columns), bf16) for size in sizes[:-1]]
        + [pltpu.VMEM((n, 1, sizes[-1], columns), bf16)]
        + [pltpu.VMEM((2, size, columns), bf16) for size in sizes]
        + [pltpu.VMEM((1, size, columns), bf16) for size in sizes]
        + [
            pltpu.VMEM((2, sizes[-1], columns), bf16),
            dma(()), dma(()),
            dma(()), dma(()),
            dma(()), dma((count,)),
            dma(()), dma((count,)),
            dma((count, 2)), dma((count, 2)),
            dma(()), dma(()), pltpu.SemaphoreType.REGULAR,
        ]
    )
    tail = sizes[-1]
    near = pl.BlockSpec(memory_space=pltpu.VMEM)
    parts = pl.pallas_call(
        functools.partial(kernel, n, lats, sizes, columns, rows),
        out_shape=(
            pltpu.VMEM((slices - tail, columns, rows), bf16),
            pltpu.VMEM((tail, rows + 2 * EDGE, columns), bf16),
            pltpu.VMEM((4, rows, columns), f32),
        ),
        in_specs=[pl.BlockSpec(memory_space=pltpu.SMEM), far, far, far, far],
        out_specs=(near,) * 3,
        scratch_shapes=scratch,
        compiler_params=pltpu.CompilerParams(
            collective_id=0, has_side_effects=True, vmem_limit_bytes=24_000_000
        ),
    )(
        sector_shift,
        *[
            pltpu.with_memory_space_constraint(value, pltpu.HBM)
            for value in (tracers.reshape(slices, columns, rows), lon_offset, lon_frac, lat_frac)
        ],
    )
    result = pl.pallas_call(
        functools.partial(finishing, rows),
        out_shape=jax.ShapeDtypeStruct((slices, columns, rows), bf16),
        in_specs=[near] * 3,
        out_specs=far,
        scratch_shapes=[
            pltpu.VMEM((tail, columns, rows), bf16),
            pltpu.VMEM((tail, rows + 2 * EDGE, columns), f32),
            dma((1 + tail // GROUP,)),
        ],
        compiler_params=pltpu.CompilerParams(vmem_limit_bytes=8_000_000),
    )(*parts)
    return result.reshape(tracers.shape)


def local(tracers, *rest):
    fields, levels, columns, rows = tracers.shape
    split = EDGE * lax.axis_size("lon")
    if columns == LANES and rows == LANES and rows % split == 0 and (fields * levels) % (10 * GROUP) == 0 and (fields * levels) % lax.axis_size("lon") == 0:
        return exchanged(tracers, *rest)
    return general(tracers, *rest)


def solution(mesh):
    return jax.shard_map(
        local,
        mesh=mesh,
        in_specs=(
            P(None, None, "lon", "lat"),
            P("lat"),
            P("lon", "lat"),
            P("lon", "lat"),
            P("lon", "lat"),
        ),
        out_specs=P(None, None, "lon", "lat"),
        check_vma=False,
    )
```

```python
import functools

import jax
import jax.numpy as jnp
from jax import lax
from jax.experimental import pallas as pl
from jax.experimental.pallas import tpu as pltpu
from jax.sharding import PartitionSpec as P

SMAX = 6
LANES = 128
EDGE = 16
STEPS = 65535.0
MIDDLE = 32768
BLOCK = 32
GROUP = 4
PARTS = (4, 2)


def shifted(value, axis, steps):
    count = lax.axis_size(axis)
    pairs = [(source, (source + steps) % count) for source in range(count)]
    return lax.ppermute(value, axis, pairs)


def padded_2(block, sides, width):
    for axis, dim in sides:
        count = lax.axis_size(axis)
        forward = [(i, i + 1) for i in range(count - 1)]
        backward = [(target, source) for source, target in forward]
        low = lax.ppermute(
            lax.slice_in_dim(block, block.shape[dim] - width, None, axis=dim), axis, forward
        )
        high = lax.ppermute(lax.slice_in_dim(block, 0, width, axis=dim), axis, backward)
        block = jnp.concatenate([low, block, high], axis=dim)
    return block


def lagrange(position):
    return (
        -position * (position - 1.0) * (position - 2.0) / 6.0,
        (position + 1.0) * (position - 1.0) * (position - 2.0) / 2.0,
        -(position + 1.0) * position * (position - 2.0) / 2.0,
        (position + 1.0) * position * (position - 1.0) / 6.0,
    )


def general(tracers, sector_shift, lon_offset, lon_frac, lat_frac):
    fields, levels, columns_here, rows_here = tracers.shape
    stacked = tracers.reshape(fields * levels, columns_here, rows_here)
    shift_count = sector_shift[0]
    nothing = jnp.zeros((), jnp.bfloat16)
    lon_weights = [weight.astype(jnp.bfloat16) for weight in lagrange(lon_frac)]
    window_rows = lax.broadcasted_iota(jnp.int32, (2 * columns_here, columns_here, rows_here), 0)
    column_index = lax.broadcasted_iota(jnp.int32, (columns_here, rows_here), 0)
    lon_matrix = jnp.zeros((2 * columns_here, columns_here, rows_here), jnp.bfloat16)
    for stencil in range(4):
        target = column_index - lon_offset + (stencil - 1 + columns_here)
        lon_matrix = lon_matrix + jnp.where(
            window_rows == target[None], lon_weights[stencil][None], nothing
        )
    lat_weights = [weight.astype(jnp.bfloat16).astype(jnp.float32) for weight in lagrange(lat_frac)]
    nearer = stacked
    for bit_place in range(SMAX.bit_length()):
        arrived = shifted(nearer, "lon", 1 << bit_place)
        nearer = jnp.where((shift_count >> bit_place) % 2 == 1, arrived, nearer)
    farther = shifted(nearer, "lon", 1)
    window = jnp.concatenate((farther, nearer), axis=1)
    between = jnp.einsum(
        "bjr,jor->bor", window, lon_matrix, preferred_element_type=jnp.float32
    ).astype(jnp.bfloat16)
    padded = padded_2(between, (("lat", 2),), 2)
    result = jnp.zeros(between.shape, jnp.float32)
    for stencil in range(4):
        result = result + lat_weights[stencil][None] * padded[
            :, :, 1 + stencil : 1 + stencil + rows_here
        ].astype(jnp.float32)
    return result.astype(jnp.bfloat16).reshape(fields, levels, columns_here, rows_here)


def blended(weights_ref, wide, rows):
    totals = [[] for _ in range(wide.shape[0])]
    for row in range(0, rows, BLOCK):
        weights = [weights_ref[tap, row : row + BLOCK] for tap in range(4)]
        for which, parts in enumerate(totals):
            total = weights[0] * wide[which, pl.ds(EDGE - 1 + row, BLOCK)]
            for tap in range(1, 4):
                total = total + weights[tap] * wide[which, pl.ds(EDGE - 1 + tap + row, BLOCK)]
            parts.append(total)
    return [jnp.concatenate(parts, axis=0).astype(jnp.bfloat16).T for parts in totals]


def kernel(n, lats, sizes, columns, rows, *refs):
    count = len(sizes)
    starts = [sum(sizes[:chunk]) for chunk in range(count)]
    share = rows // n
    last = count - 1
    shift_ref, tracer_ref, offset_ref, lon_ref, lat_ref, ready, home_last, lat_weights = refs[:8]
    refs = refs[8:]
    sent, refs = refs[:count], refs[count:]
    taken, refs = refs[:count], refs[count:]
    mixed, refs = refs[:count], refs[count:]
    home, refs = refs[:last] + (home_last,), refs[last:]
    raw, offset, lon_part, lat_part, coded, code, first, lon_weights, wide = refs[:9]
    refs = refs[9:]
    low, refs = refs[:count], refs[count:]
    high, refs = refs[:count], refs[count:]
    above, refs = refs[:count], refs[count:]
    below, refs = refs[:count], refs[count:]
    relay, refs = refs[0], refs[1:]
    (load_sem, part_sem, code_send, code_recv, take_send, take_recv, home_send, home_recv,
     edge_send, edge_recv, rim_send, rim_recv, open_sem) = refs

    me = lax.axis_index("lon")
    band = lax.axis_index("lat")
    bar = pltpu.get_barrier_semaphore()
    f32, bf16 = jnp.float32, jnp.bfloat16

    def partner(step):
        if n != 8:
            return lax.rem(me + step, n)
        at = step - 1
        pair = 6 - 2 * (at // 2) + at - 2 * (at // 2)
        mask = pair + at // 6 * (1 - 2 * pair)
        flips = [lax.rem(mask // bit, 2) for bit in (1, 2, 4)]
        mine = [lax.rem(me // bit, 2) for bit in (1, 2, 4)]
        flips[2] = lax.rem(flips[2] + flips[1] * mine[0], 2)
        return sum(bit * lax.rem(flip + own, 2) for bit, flip, own in zip((1, 2, 4), flips, mine))

    def shared(owner):
        return pl.ds(pl.multiple_of((n - 1 - owner) * share, share), share)

    def landed(owner):
        return pl.ds(pl.multiple_of(EDGE + (n - 1 - owner) * share, EDGE), share)

    def part_copy(place):
        return pltpu.make_async_copy(
            (offset_ref, lon_ref, lat_ref)[place], (offset, lon_part, lat_part)[place], part_sem
        )

    def every_part():
        parts = lat_weights.at[pl.ds(0, 3)]
        return pltpu.make_async_copy(parts, parts, part_sem)

    def load_copy():
        return pltpu.make_async_copy(tracer_ref, raw, load_sem)

    def code_copy(step):
        return pltpu.make_async_remote_copy(
            src_ref=coded.at[:, shared(partner(step))], dst_ref=code.at[me],
            send_sem=code_send, recv_sem=code_recv,
            device_id={"lon": partner(step)},
        )

    def take_copy(chunk, step):
        return pltpu.make_async_remote_copy(
            src_ref=sent[chunk].at[:, shared(partner(step))], dst_ref=taken[chunk].at[me],
            send_sem=take_send, recv_sem=take_recv.at[chunk],
            device_id={"lon": partner(step)},
        )

    def home_copy(chunk, step):
        return pltpu.make_async_remote_copy(
            src_ref=mixed[chunk].at[partner(step)], dst_ref=home[chunk].at[:, landed(me)],
            send_sem=home_send, recv_sem=home_recv.at[chunk],
            device_id={"lon": partner(step)},
        )

    def every(block, send_sem, recv_sem):
        part = block.at[pl.ds(0, n - 1)]
        return pltpu.make_async_remote_copy(
            src_ref=part, dst_ref=part, send_sem=send_sem, recv_sem=recv_sem,
            device_id={"lon": partner(1)},
        )

    def every_code():
        return every(code, code_send, code_recv)

    def every_take(chunk):
        return every(taken[chunk], take_send, take_recv.at[chunk])

    def every_home(chunk):
        return every(mixed[chunk], home_send, home_recv.at[chunk])

    def every_send(send_sem):
        part = raw.at[pl.ds(0, raw.shape[0] // n * (n - 1))]
        return pltpu.make_async_remote_copy(
            src_ref=part, dst_ref=part, send_sem=send_sem, recv_sem=take_recv.at[0],
            device_id={"lon": partner(1)},
        )

    def bottom_edge(chunk):
        return pltpu.make_async_remote_copy(
            src_ref=low[chunk] if chunk < last else relay, dst_ref=above[chunk],
            send_sem=edge_send.at[0], recv_sem=edge_recv.at[chunk, 0],
            device_id={"lat": band - 1},
        )

    def top_edge(chunk):
        return pltpu.make_async_remote_copy(
            src_ref=high[chunk], dst_ref=below[chunk],
            send_sem=edge_send.at[1], recv_sem=edge_recv.at[chunk, 1],
            device_id={"lat": band + 1},
        )

    def every_edge(side, lines):
        part = raw.at[0, pl.ds(0, lines)]
        return pltpu.make_async_remote_copy(
            src_ref=part, dst_ref=part, send_sem=edge_send.at[side], recv_sem=edge_recv.at[0, side],
            device_id={"lat": band + 2 * side - 1},
        )

    def bottom_copy(step):
        return pltpu.make_async_remote_copy(
            src_ref=low[last].at[partner(step)], dst_ref=relay,
            send_sem=rim_send, recv_sem=rim_recv,
            device_id={"lon": partner(step)},
        )

    def top_copy(sector):
        return pltpu.make_async_remote_copy(
            src_ref=high[last].at[sector], dst_ref=below[last],
            send_sem=rim_send, recv_sem=edge_recv.at[last, 1],
            device_id={"lat": band + 1, "lon": sector},
        )

    def every_top():
        return pltpu.make_async_remote_copy(
            src_ref=high[last], dst_ref=high[last], send_sem=rim_send, recv_sem=edge_recv.at[last, 1],
            device_id={"lat": band + 1},
        )

    gives_bottom = jnp.logical_and(me == n - 1, band > 0)
    gives_top = jnp.logical_and(me == 0, band < lats - 1)

    for step in range(1, n):
        pl.semaphore_signal(bar, inc=1, device_id={"lon": partner(step)})

    @pl.when(band > 0)
    def _():
        pl.semaphore_signal(bar, inc=1, device_id={"lat": band - 1})

    @pl.when(band < lats - 1)
    def _():
        pl.semaphore_signal(bar, inc=1, device_id={"lat": band + 1})

    part_copy(0).start()
    part_copy(1).start()
    part_copy(2).start()
    load_copy().start()

    def turn(chunk):
        for place in range(sizes[chunk]):
            sent[chunk][place] = raw[starts[chunk] + place].T
        taken[chunk][me] = sent[chunk][:, shared(me)]

    every_part().wait()
    coded[0] = offset[...].T.astype(jnp.int16)
    level = jnp.floor(lon_part[...].T * STEPS + 0.5).astype(jnp.int32) - MIDDLE
    coded[1] = level.astype(jnp.int16)
    code[me] = coded[:, shared(me)]

    sides = jnp.where(band > 0, 1, 0) + jnp.where(band < lats - 1, 1, 0)
    with jax.named_scope("bar"):
        pl.semaphore_wait(bar, n - 1 + sides)
    for step in range(1, n):
        code_copy(step).start()
    load_copy().wait()
    for chunk in range(count):
        turn(chunk)
        for step in range(1, n):
            take_copy(chunk, step).start()

    @pl.when(jnp.logical_and(me == 0, band > 0))
    def _():
        pl.semaphore_signal(open_sem, inc=1, device_id={"lat": band - 1})

    for tap, weight in enumerate(lagrange(lat_part[...].T)):
        lat_weights[tap] = weight.astype(bf16).astype(f32)
    for chunk in range(count):
        @pl.when(band == 0)
        def _():
            home[chunk][:, 0:EDGE] = jnp.zeros((sizes[chunk], EDGE, columns), bf16)

        @pl.when(band == lats - 1)
        def _():
            home[chunk][:, EDGE + rows:] = jnp.zeros((sizes[chunk], EDGE, columns), bf16)

    every_code().wait_recv()

    def prepare(sector, carry):
        lane = lax.broadcasted_iota(jnp.int32, (share, columns), 1)
        first[sector] = lane - code[sector, 0].astype(jnp.int32) + (columns - 1)
        level = code[sector, 1].astype(jnp.int32) + MIDDLE
        position = level.astype(f32) * (1.0 / STEPS)
        for tap, weight in enumerate(lagrange(position)):
            lon_weights[tap, sector] = weight.astype(bf16).astype(f32)
        return carry

    lax.fori_loop(0, n, prepare, 0)
    shift_count = shift_ref[0]

    def along_lon(chunk, sector):
        near_at = lax.rem(sector - shift_count + 8 * n, n)
        far_at = lax.rem(sector - shift_count - 1 + 8 * n, n)
        near = [taken[chunk][near_at, place].astype(f32) for place in range(sizes[chunk])]
        far = [taken[chunk][far_at, place].astype(f32) for place in range(sizes[chunk])]
        totals = [[] for _ in near]
        for row in range(0, share, 8):
            part = slice(row, row + 8)
            base = first[sector, part]
            sums = [None] * len(near)
            for tap in range(4):
                spot = base + tap if tap else base
                lane = spot & (columns - 1)
                nearer = spot >= columns
                weight = lon_weights[tap, sector, part]
                for place in range(len(near)):
                    picked = jnp.where(
                        nearer,
                        jnp.take_along_axis(near[place][part], lane, axis=1, mode="promise_in_bounds"),
                        jnp.take_along_axis(far[place][part], lane, axis=1, mode="promise_in_bounds"),
                    )
                    term = weight * picked
                    sums[place] = term if tap == 0 else sums[place] + term
            for place, total in enumerate(sums):
                totals[place].append(total)
        for place, parts in enumerate(totals):
            mixed[chunk][sector, place] = jnp.concatenate(parts, axis=0).astype(bf16)

    for chunk in range(count):
        with jax.named_scope(f"take{chunk}"):
            every_take(chunk).wait_recv()

        def send(turn_of, carry):
            step = turn_of
            along_lon(chunk, partner(step))

            @pl.when(step < n if chunk == 0 else jnp.logical_and(step < n, jnp.logical_not(gives_bottom)))
            def _():
                home_copy(chunk, step).start()
            return carry

        with jax.named_scope(f"lon{chunk}"):
            lax.fori_loop(1, n + 1, send, 0)
        home[chunk][:, landed(me)] = mixed[chunk][me]

    @pl.when(gives_bottom)
    def _():
        def give(step, carry):
            sector = partner(step)
            rows_of = mixed[last][sector].astype(f32)
            for row in range(2):
                low[last][sector, row] = rows_of[:, row].astype(bf16)

            @pl.when(step < n)
            def _():
                bottom_copy(step).start()
            return carry

        lax.fori_loop(1, n + 1, give, 0)
        relay[...] = low[last][me]
        for chunk in range(1, count):
            def late(step, carry):
                home_copy(chunk, step).start()
                return carry

            lax.fori_loop(1, n, late, 0)

    @pl.when(gives_top)
    def _():
        pl.semaphore_wait(open_sem, 1)

        def give(sector, carry):
            high[last][sector, 0] = mixed[last][sector].astype(f32)[:, share - 1].astype(bf16)
            top_copy(sector).start()
            return carry

        lax.fori_loop(0, n, give, 0)

    def send_edges(chunk):
        @pl.when(band > 0)
        def _():
            rows_of = home[chunk][:, EDGE : 2 * EDGE].astype(f32)
            for row in range(2):
                low[chunk][row] = rows_of[:, row].astype(bf16)
            bottom_edge(chunk).start()

        @pl.when(band < lats - 1)
        def _():
            rows_of = home[chunk][:, rows : EDGE + rows].astype(f32)
            high[chunk][0] = rows_of[:, EDGE - 1].astype(bf16)
            top_edge(chunk).start()

    def take_edges(chunk):
        @pl.when(band > 0)
        def _():
            (top_edge(chunk) if chunk < last else top_copy(0)).wait_recv()
            row = below[chunk][0].astype(f32)
            for place in range(sizes[chunk]):
                home[chunk][place, 0:EDGE] = jnp.broadcast_to(
                    row[place : place + 1], (EDGE, columns)
                ).astype(bf16)

        @pl.when(band < lats - 1)
        def _():
            bottom_edge(chunk).wait_recv()
            near, far = above[chunk][0].astype(f32), above[chunk][1].astype(f32)
            nearest = lax.broadcasted_iota(jnp.int32, (EDGE, columns), 0) == 0
            for place in range(sizes[chunk]):
                home[chunk][place, EDGE + rows :] = jnp.where(
                    nearest, near[place : place + 1], far[place : place + 1]
                ).astype(bf16)

    def along_lat(chunk):
        def finish(group, carry):
            first_place = group * GROUP
            for which in range(GROUP):
                wide[which] = home[chunk][first_place + which].astype(f32)
            for which, block in enumerate(blended(lat_weights, wide, rows)):
                ready[starts[chunk] + first_place + which] = block
            return carry

        with jax.named_scope(f"lat{chunk}"):
            lax.fori_loop(0, sizes[chunk] // GROUP, finish, 0)

    every_code().wait_send()
    for chunk in range(count):
        with jax.named_scope(f"home{chunk}"):
            every_home(chunk).wait_recv()
        if chunk < last:
            if chunk == 0:
                with jax.named_scope("relay"):
                    @pl.when(jnp.logical_and(band > 0, me < n - 1))
                    def _():
                        bottom_copy(1).wait_recv()

                    @pl.when(band > 0)
                    def _():
                        bottom_edge(last).start()
            send_edges(chunk)
            if chunk == last - 1:
                take_edges(last)
            with jax.named_scope(f"edges{chunk}"):
                take_edges(chunk)
            along_lat(chunk)

    with jax.named_scope("sends"):
        every_send(take_send).wait_send()
        every_send(home_send).wait_send()

        @pl.when(band > 0)
        def _():
            every_edge(0, 2 * sum(sizes)).wait_send()

        @pl.when(band < lats - 1)
        def _():
            every_edge(1, sum(sizes[:last])).wait_send()

        @pl.when(gives_bottom)
        def _():
            every(low[last], rim_send, rim_recv).wait_send()

        @pl.when(gives_top)
        def _():
            every_top().wait_send()


def finishing(rows, ready_ref, home_ref, weights_ref, out_ref, done, wide, sem):
    head, tail = ready_ref.shape[0], home_ref.shape[0]
    copies = []

    def put(source, place, size):
        copy = pltpu.make_async_copy(source, out_ref.at[pl.ds(place, size)], sem.at[len(copies)])
        copy.start()
        copies.append(copy)

    put(ready_ref, 0, head)
    for group in range(0, tail, GROUP):
        part = wide.at[pl.ds(group, GROUP)]
        for which in range(GROUP):
            part[which] = home_ref[group + which].astype(jnp.float32)
        for which, block in enumerate(blended(weights_ref, part, rows)):
            done[group + which] = block
        put(done.at[pl.ds(group, GROUP)], head + group, GROUP)
    for copy in copies:
        copy.wait()


def exchanged(tracers, sector_shift, lon_offset, lon_frac, lat_frac):
    fields, levels, columns, rows = tracers.shape
    n, lats = lax.axis_size("lon"), lax.axis_size("lat")
    slices = fields * levels
    leading = [slices * part // 40 * GROUP for part in PARTS]
    sizes = [size for size in leading + [slices - sum(leading)] if size]
    share = rows // n
    f32, bf16 = jnp.float32, jnp.bfloat16
    dma = pltpu.SemaphoreType.DMA
    count = len(sizes)
    far = pl.BlockSpec(memory_space=pltpu.HBM)
    scratch = (
        [pltpu.VMEM((size, rows, columns), bf16) for size in sizes]
        + [pltpu.VMEM((n, size, share, columns), bf16) for size in sizes]
        + [pltpu.VMEM((n, size, share, columns), bf16) for size in sizes]
        + [pltpu.VMEM((size, rows + 2 * EDGE, columns), bf16) for size in sizes[:-1]]
        + [
            pltpu.VMEM((slices, columns, rows), bf16),
            pltpu.VMEM((columns, rows), jnp.int32),
            pltpu.VMEM((columns, rows), f32),
            pltpu.VMEM((columns, rows), f32),
            pltpu.VMEM((2, rows, columns), jnp.int16),
            pltpu.VMEM((n, 2, share, columns), jnp.int16),
            pltpu.VMEM((n, share, columns), jnp.int32),
            pltpu.VMEM((4, n, share, columns), f32),
            pltpu.VMEM((GROUP, rows + 2 * EDGE, columns), f32),
        ]
        + [pltpu.VMEM((2, size, columns), bf16) for size in sizes[:-1]]
        + [pltpu.VMEM((n, 2, sizes[-1], columns), bf16)]
        + [pltpu.VMEM((1, size, columns), bf16) for size in sizes[:-1]]
        + [pltpu.VMEM((n, 1, sizes[-1], columns), bf16)]
        + [pltpu.VMEM((2, size, columns), bf16) for size in sizes]
        + [pltpu.VMEM((1, size, columns), bf16) for size in sizes]
        + [
            pltpu.VMEM((2, sizes[-1], columns), bf16),
            dma(()), dma(()),
            dma(()), dma(()),
            dma(()), dma((count,)),
            dma(()), dma((count,)),
            dma((2,)), dma((count, 2)),
            dma(()), dma(()), pltpu.SemaphoreType.REGULAR,
        ]
    )
    tail = sizes[-1]
    near = pl.BlockSpec(memory_space=pltpu.VMEM)
    parts = pl.pallas_call(
        functools.partial(kernel, n, lats, sizes, columns, rows),
        out_shape=(
            pltpu.VMEM((slices - tail, columns, rows), bf16),
            pltpu.VMEM((tail, rows + 2 * EDGE, columns), bf16),
            pltpu.VMEM((4, rows, columns), f32),
        ),
        in_specs=[pl.BlockSpec(memory_space=pltpu.SMEM), far, far, far, far],
        out_specs=(near,) * 3,
        scratch_shapes=scratch,
        compiler_params=pltpu.CompilerParams(
            collective_id=0, has_side_effects=True, vmem_limit_bytes=24_000_000
        ),
    )(
        sector_shift,
        *[
            pltpu.with_memory_space_constraint(value, pltpu.HBM)
            for value in (tracers.reshape(slices, columns, rows), lon_offset, lon_frac, lat_frac)
        ],
    )
    result = pl.pallas_call(
        functools.partial(finishing, rows),
        out_shape=jax.ShapeDtypeStruct((slices, columns, rows), bf16),
        in_specs=[near] * 3,
        out_specs=far,
        scratch_shapes=[
            pltpu.VMEM((tail, columns, rows), bf16),
            pltpu.VMEM((tail, rows + 2 * EDGE, columns), f32),
            dma((1 + tail // GROUP,)),
        ],
        compiler_params=pltpu.CompilerParams(vmem_limit_bytes=8_000_000),
    )(*parts)
    return result.reshape(tracers.shape)


def local(tracers, *rest):
    fields, levels, columns, rows = tracers.shape
    split = EDGE * lax.axis_size("lon")
    if columns == LANES and rows == LANES and rows % split == 0 and (fields * levels) % (10 * GROUP) == 0 and (fields * levels) % lax.axis_size("lon") == 0:
        return exchanged(tracers, *rest)
    return general(tracers, *rest)


def solution(mesh):
    return jax.shard_map(
        local,
        mesh=mesh,
        in_specs=(
            P(None, None, "lon", "lat"),
            P("lat"),
            P("lon", "lat"),
            P("lon", "lat"),
            P("lon", "lat"),
        ),
        out_specs=P(None, None, "lon", "lat"),
        check_vma=False,
    )
```
